32 devices in a mesh: fsdp: 4 (over y, x), seq: 8 (over z, core).
Axes of the slice: x: 2, y: 2, z: 4, core: 2. Of those that a mesh axis runs over, the one named last changes fastest.
Arguments:
- images: bfloat16 [32, 1024, 1152], P('fsdp', 'seq'), may hold values from -8 to 8
- lengths: int32 [32], P('fsdp'), may hold values from 256 to 1024
- ln1_gain: bfloat16 [1152], P('fsdp'), may hold values from 0.099609375 to 1.8984375
- ln1_bias: bfloat16 [1152], P('fsdp'), may hold values from -3 to 3
- w_qkv: bfloat16 [1152, 3456], P('fsdp'), may hold values from -1 to 1
- qv_bias: bfloat16 [2, 1152], P(None, 'fsdp'), may hold values from -3 to 3
- w_out: bfloat16 [1152, 1152], P('fsdp'), may hold values from -0.75 to 0.75
- out_bias: bfloat16 [1152], P('fsdp'), may hold values from -3 to 3
- ln2_gain: bfloat16 [1152], P('fsdp'), may hold values from 0.099609375 to 1.8984375
- ln2_bias: bfloat16 [1152], P('fsdp'), may hold values from -3 to 3
- w_up: bfloat16 [1152, 4304], P('fsdp'), may hold values from -0.1875 to 0.1875
- up_bias: bfloat16 [4304], P('fsdp'), may hold values from -3 to 3
- w_down: bfloat16 [4304, 1152], P(None, 'fsdp'), may hold values from -0.09375 to 0.09375
- down_bias: bfloat16 [1152], P('fsdp'), may hold values from -3 to 3
- cotangent: bfloat16 [32, 1024, 1152], P('fsdp', 'seq'), may hold values from -6 to 6
Outputs:
- layer_out: bfloat16 [32, 1024, 1152], P('fsdp', 'seq')
- grad_images: bfloat16 [32, 1024, 1152], P('fsdp', 'seq')
- grad_ln1_gain: float32 [1152], P('fsdp')
- grad_ln1_bias: float32 [1152], P('fsdp')
- grad_w_qkv: float32 [1152, 3456], P('fsdp')
- grad_qv_bias: float32 [2, 1152], P(None, 'fsdp')
- grad_w_out: float32 [1152, 1152], P('fsdp')
- grad_out_bias: float32 [1152], P('fsdp')
- grad_ln2_gain: float32 [1152], P('fsdp')
- grad_ln2_bias: float32 [1152], P('fsdp')
- grad_w_up: float32 [1152, 4304], P('fsdp')
- grad_up_bias: float32 [4304], P('fsdp')
- grad_w_down: float32 [4304, 1152], P(None, 'fsdp')
- grad_down_bias: float32 [1152], P('fsdp')
The draws below stay inside these ranges and needn't reach their ends.
All inputs are finite; a program needn't handle non-finite values.
Results may differ from the reference program's by a relative error of at most 0.017.
Values may be sent and summed in bfloat16 or wider, within the bound.
A program may use at most 256 MiB of HBM per device.

```python
import math
import jax
import jax.numpy as jnp
from jax import lax

D = 1152
H = 16
HD = 72
FF = 4304
LEN = 1024
IMAGES = 32


def draw_lengths(key, part):
    key_first, key_second = jax.random.split(jax.random.fold_in(key, 11))
    drawn = jax.random.randint(key_first, (IMAGES,), LEN // 4, LEN + 1)
    position = jax.random.randint(key_second, (), 0, IMAGES)
    return jnp.where(jnp.arange(IMAGES) == position, LEN, drawn).astype(jnp.int32)


def draw_images(key, part):
    source = jax.random.fold_in(key, 23)
    samples = jax.random.normal(source, (IMAGES, LEN, D), jnp.float32)
    return jnp.clip(samples, -8.0, 8.0).astype(jnp.bfloat16)


def draw_w_qkv(key, part):
    source = jax.random.fold_in(key, 37)
    baseline = jax.random.normal(source, (D, 3 * D), jnp.float32) * D ** (-0.5)
    return jnp.clip(baseline, -1.0, 1.0).astype(jnp.bfloat16)


def block_scale(key, extent, shards, smallest, top_value):
    factor_of = 1.0
    for dim, parts in shards:
        draws = jax.random.uniform(jax.random.fold_in(jax.random.fold_in(key, 6), dim), (parts,), jnp.float32, smallest / len(shards), top_value / len(shards))
        factor_of = factor_of * jnp.repeat(jnp.exp(draws), extent[dim] // parts).reshape((-1,) + (1,) * (len(extent) - 1 - dim))
    return factor_of


def gaussian(rng, shape, deviation, reach, cuts=(), kind=jnp.bfloat16):
    array = deviation * jax.random.normal(rng, shape, jnp.float32)
    if cuts:
        array = array * block_scale(rng, shape, cuts, -0.22, 0.18)
    return jnp.clip(array, -reach, reach).astype(kind)


def setup_inputs(seed: int = 0) -> dict:
    key_list = jax.random.split(jax.random.key(seed), 16)
    return {
        "images": draw_images(jax.random.fold_in(key_list[15], 71), 0),
        "lengths": draw_lengths(jax.random.fold_in(key_list[15], 71), 0),
        "ln1_gain": jnp.clip(1.0 + 0.18 * jax.random.normal(key_list[2], (D,), jnp.float32), 0.099609375, 1.8984375).astype(jnp.bfloat16),
        "ln1_bias": gaussian(key_list[3], (D,), 0.5, 3.0, ((0, 4),)),
        "w_qkv": draw_w_qkv(jax.random.fold_in(key_list[15], 71), 0),
        "qv_bias": gaussian(key_list[5], (2, D), 0.5, 3.0, ((1, 4),)),
        "w_out": gaussian(key_list[6], (D, D), (D // 16) ** -0.5, 0.75, ((0, 4),)),
        "out_bias": gaussian(key_list[7], (D,), 0.5, 3.0, ((0, 4),)),
        "ln2_gain": jnp.clip(1.0 + 0.18 * jax.random.normal(key_list[8], (D,), jnp.float32), 0.099609375, 1.8984375).astype(jnp.bfloat16),
        "ln2_bias": gaussian(key_list[9], (D,), 0.5, 3.0, ((0, 4),)),
        "w_up": gaussian(key_list[10], (D, FF), D ** -0.5, 0.1875, ((0, 4),)),
        "up_bias": gaussian(key_list[11], (FF,), 0.5, 3.0, ((0, 4),)),
        "w_down": gaussian(key_list[12], (FF, D), FF ** -0.5, 0.09375, ((1, 4),)),
        "down_bias": gaussian(key_list[13], (D,), 0.5, 3.0, ((0, 4),)),
        "cotangent": gaussian(key_list[14], (IMAGES, LEN, D), 1.0, 6.0, ((0, 4), (1, 8))),
    }


epsilon = 1e-06
highest = lax.Precision.HIGHEST

@jax.custom_vjp
def low(v):
    return lax.optimization_barrier(v.astype(jnp.bfloat16)).astype(jnp.float32)

@jax.custom_vjp
def low_back(v):
    return v

def low_keep(v):
    return (low(v), None)

def low_pass(kept, grad):
    return (grad,)

def back_keep(v):
    return (v, None)

def back_low(kept, grad):
    return (low(grad),)
low.defvjp(low_keep, low_pass)
low_back.defvjp(back_keep, back_low)

def normalize(field, gain_vec, bias_vec):
    center_mean = lax.optimization_barrier(jnp.mean(field, -1, keepdims=True))
    centered = field - center_mean
    variance = lax.optimization_barrier(jnp.mean(centered * centered, -1, keepdims=True))
    return centered * lax.rsqrt(variance + epsilon) * gain_vec + bias_vec

def attend_block(queries, keys_all, values, visible):
    scores = low_back(jnp.dot(queries, keys_all.T, precision=highest))
    scores = jnp.where(visible[None, :], scores, -1e+30)
    softmax_out = jax.nn.softmax(scores, axis=-1)
    return jnp.dot(low(softmax_out), values, precision=highest)

def attend_one(packed):
    queries, keys_all, values, length_one = packed
    length_all = keys_all.shape[0]
    block_rows = min(1024, length_all)
    visible = jnp.arange(length_all) < length_one
    pieces = [jax.checkpoint(attend_block)(queries[offset:offset + block_rows], keys_all, values, visible) for offset in range(0, length_all, block_rows)]
    return jnp.concatenate(pieces, 0)

def layer(inputs_all, lengths_group, params):
    gain_one, bias_one, qkv_weight, qv_shift, out_weight, out_shift, gain_two, bias_two, up_weight, up_shift, down_weight, down_shift = params
    group_size, length_all, width_all = inputs_all.shape
    normed_attn = low(normalize(inputs_all, gain_one, bias_one))
    projected = jnp.einsum('gtd,dc->gtc', normed_attn, qkv_weight, precision=highest).reshape(group_size, length_all, 3, H, HD)
    head_scale = HD ** (-0.5)
    queries = low(low_back((projected[:, :, 0] + qv_shift[0].reshape(H, HD)) * head_scale))
    keys_all = low(low_back(projected[:, :, 1]))
    values = low(low_back(projected[:, :, 2] + qv_shift[1].reshape(H, HD)))

    def as_items(field):
        return field.transpose(0, 2, 1, 3).reshape(group_size * H, length_all, HD)
    lengths_rep = jnp.repeat(lengths_group, H)
    attended = lax.map(attend_one, (as_items(queries), as_items(keys_all), as_items(values), lengths_rep))
    attended = attended.reshape(group_size, H, length_all, HD).transpose(0, 2, 1, 3).reshape(group_size, length_all, width_all)
    attended = low(low_back(attended))
    residual = inputs_all + low_back(jnp.einsum('gtd,de->gte', attended, out_weight, precision=highest) + out_shift)
    normed_mlp = low(normalize(residual, gain_two, bias_two))
    pre_act = low_back(jnp.einsum('gtd,df->gtf', normed_mlp, up_weight, precision=highest) + up_shift)
    activation = low(jax.nn.gelu(pre_act, approximate=True))
    return residual + jnp.einsum('gtf,fd->gtd', activation, down_weight, precision=highest) + down_shift

def reference(images, lengths, ln1_gain, ln1_bias, w_qkv, qv_bias, w_out, out_bias, ln2_gain, ln2_bias, w_up, up_bias, w_down, down_bias, cotangent):
    params = tuple((p.astype(jnp.float32) for p in (ln1_gain, ln1_bias, w_qkv, qv_bias, w_out, out_bias, ln2_gain, ln2_bias, w_up, up_bias, w_down, down_bias)))
    group_size = math.gcd(IMAGES, max(1, 4096 // LEN))
    group_count = IMAGES // group_size
    inputs_all = images.astype(jnp.float32).reshape(group_count, group_size, LEN, D)
    lengths_all = lengths.reshape(group_count, group_size)
    cot_all = cotangent.astype(jnp.float32).reshape(group_count, group_size, LEN, D)

    def scan_step(running, portion):
        inputs_group, lengths_group, cot_group = portion
        output_group, pullback = jax.vjp(lambda field, weights: layer(field, lengths_group, weights), inputs_group, params)
        grad_inputs, grad_params = pullback(cot_group)
        return (tuple((left + right for left, right in zip(running, grad_params))), (output_group, grad_inputs))
    zero_grads = tuple((jnp.zeros(p.shape, p.dtype) for p in params))
    totals, (outputs, grad_inputs) = lax.scan(scan_step, zero_grads, (inputs_all, lengths_all, cot_all))
    return (outputs.reshape(IMAGES, LEN, D).astype(jnp.bfloat16), grad_inputs.reshape(IMAGES, LEN, D).astype(jnp.bfloat16), totals[0], totals[1], totals[2], totals[3], totals[4], totals[5], totals[6], totals[7], totals[8], totals[9], totals[10], totals[11])
```

```python
import functools
import math

import jax
import jax.numpy as jnp
from jax import lax
from jax.experimental import pallas as pl
from jax.experimental.pallas import tpu as pltpu
from jax.sharding import Mesh
from jax.sharding import PartitionSpec as P

H = 16
HD = 72
WIDTH = H * HD
EPS = 1e-06
LOG2E = math.log2(math.e)
BF = jnp.bfloat16
F32 = jnp.float32
SEQ = ("z", "core")


def nt(a, b):
    return lax.dot_general(a, b, (((1,), (1,)), ((), ())), preferred_element_type=F32)


def nn(a, b):
    return lax.dot_general(a, b, (((1,), (0,)), ((), ())), preferred_element_type=F32)


def tn(a, b):
    return lax.dot_general(a, b, (((0,), (0,)), ((), ())), preferred_element_type=F32)


def head_window(h):
    start = jnp.minimum((h * HD) // 128 * 128, WIDTH - 256)
    offset = h * HD - start
    lane = lax.broadcasted_iota(jnp.int32, (1, 256), 1)
    return pl.multiple_of(start, 128), (lane >= offset) & (lane < offset + HD)


def forward_kernel(block, q_ref, k_ref, v_ref, bias_ref, out_ref, lse_ref, total, stats):
    h = pl.program_id(0)

    @pl.when(h == 0)
    def _():
        total[...] = jnp.zeros_like(total)
        stats[...] = jnp.zeros_like(stats)

    start, mask = head_window(h)
    window = pl.ds(start, 256)
    k = k_ref[:, window]
    v = v_ref[:, window]
    bias = bias_ref[...]
    mine = lax.broadcasted_iota(jnp.int32, (1, 128), 1) == h
    for b in range(q_ref.shape[0] // block):
        rows = pl.ds(b * block, block)
        q = jnp.where(mask, q_ref[rows, window], 0)
        scores = nt(q, k) + bias
        top = jnp.max(scores, -1, keepdims=True)
        weights = jnp.exp2(scores - top)
        norm = jnp.sum(weights, -1, keepdims=True)
        mixed = nn(weights.astype(BF), v)
        total[rows, window] += jnp.where(mask, mixed * (1.0 / norm), 0.0)
        stats[rows, :] += jnp.where(mine, top + jnp.log2(norm), 0.0)

    @pl.when(h == H - 1)
    def _():
        out_ref[...] = total[...].astype(out_ref.dtype)
        lse_ref[...] = stats[...].T[:H]


def column_block(rows, index):
    return pl.BlockSpec((rows, WIDTH), lambda h: (0, index))


def whole(shape):
    return pl.BlockSpec(shape, lambda h: (0,) * len(shape))


def attend(qkv, keys, values, places, bias):
    tokens, key_count = qkv.shape[0], keys.shape[0]
    return pl.pallas_call(
        functools.partial(forward_kernel, 256),
        grid=(H,),
        in_specs=[
            column_block(tokens, 0),
            column_block(key_count, places[0]),
            column_block(key_count, places[1]),
            whole((1, key_count)),
        ],
        out_specs=[whole((tokens, WIDTH)), whole((H, tokens))],
        out_shape=[
            jax.ShapeDtypeStruct((tokens, WIDTH), BF),
            jax.ShapeDtypeStruct((H, tokens), F32),
        ],
        scratch_shapes=[pltpu.VMEM((tokens, WIDTH), F32), pltpu.VMEM((tokens, 128), F32)],
        compiler_params=pltpu.CompilerParams(
            dimension_semantics=("arbitrary",), vmem_limit_bytes=60 << 20
        ),
        cost_estimate=pl.CostEstimate(
            flops=4 * H * tokens * key_count * 256,
            bytes_accessed=8 * tokens * WIDTH,
            transcendentals=H * tokens * key_count,
        ),
        name="attend",
    )(qkv, keys, values, bias)


def backward_kernel(
    block,
    q_ref,
    k_ref,
    v_ref,
    grad_ref,
    lse_ref,
    delta_ref,
    bias_ref,
    dq_ref,
    dk_ref,
    dv_ref,
    dq_sum,
    dk_sum,
    dv_sum,
):
    h = pl.program_id(0)

    @pl.when(h == 0)
    def _():
        dq_sum[...] = jnp.zeros_like(dq_sum)
        dk_sum[...] = jnp.zeros_like(dk_sum)
        dv_sum[...] = jnp.zeros_like(dv_sum)

    start, mask = head_window(h)
    window = pl.ds(start, 256)
    q = jnp.where(mask, q_ref[:, window], 0)
    grad = jnp.where(mask, grad_ref[:, window], 0)
    lse = lse_ref[pl.ds(h, 1), :]
    delta = delta_ref[pl.ds(h, 1), :]
    dq = None
    for b in range(k_ref.shape[0] // block):
        rows = pl.ds(b * block, block)
        k = jnp.where(mask, k_ref[rows, window], 0)
        v = v_ref[rows, window]
        weights = jnp.exp2(nt(k, q) + bias_ref[rows, :] - lse)
        dscores = (weights * (nt(v, grad) - delta)).astype(BF)
        dv_sum[rows, window] += nn(weights.astype(BF), grad)
        dk_sum[rows, window] += nn(dscores, q)
        part = nn(k.T, dscores)
        dq = part if dq is None else dq + part
    dq_sum[:, window] += dq.T

    @pl.when(h == H - 1)
    def _():
        dq_ref[...] = (dq_sum[...] * HD**-0.5).astype(dq_ref.dtype)
        dk_ref[...] = (dk_sum[...] * (1.0 / LOG2E)).astype(dk_ref.dtype)
        dv_ref[...] = dv_sum[...].astype(dv_ref.dtype)


def joined_kernel(*refs):
    *inputs, out_ref, dq_sum, dk_sum, dv_sum = refs
    views = [out_ref.at[:, pl.ds(i * WIDTH, WIDTH)] for i in range(3)]
    backward_kernel(256, *inputs, *views, dq_sum, dk_sum, dv_sum)


def attend_back(qkv, keys, values, places, grad, lse, delta, bias):
    tokens, key_count = qkv.shape[0], keys.shape[0]
    joined = tokens == key_count
    if joined:
        body = joined_kernel
        shapes = [(tokens, 3 * WIDTH)]
    else:
        body = functools.partial(backward_kernel, 256)
        shapes = [(tokens, WIDTH), (key_count, WIDTH), (key_count, WIDTH)]
    return pl.pallas_call(
        body,
        grid=(H,),
        in_specs=[
            column_block(tokens, 0),
            column_block(key_count, places[0]),
            column_block(key_count, places[1]),
            whole((tokens, WIDTH)),
            whole((H, tokens)),
            whole((H, tokens)),
            whole((key_count, 1)),
        ],
        out_specs=[whole(s) for s in shapes],
        out_shape=[jax.ShapeDtypeStruct(s, BF) for s in shapes],
        scratch_shapes=[
            pltpu.VMEM((tokens, WIDTH), F32),
            pltpu.VMEM((key_count, WIDTH), F32),
            pltpu.VMEM((key_count, WIDTH), F32),
        ],
        compiler_params=pltpu.CompilerParams(
            dimension_semantics=("arbitrary",), vmem_limit_bytes=62 << 20
        ),
        cost_estimate=pl.CostEstimate(
            flops=10 * H * tokens * key_count * 256,
            bytes_accessed=14 * tokens * WIDTH,
            transcendentals=H * tokens * key_count,
        ),
        name="attend_back",
    )(qkv, keys, values, grad, lse, delta, bias)


def normal(field):
    mean = jnp.mean(field, -1, keepdims=True)
    centered = field - mean
    rate = lax.rsqrt(jnp.mean(centered * centered, -1, keepdims=True) + EPS)
    return centered * rate, rate


def normal_back(upstream, gain, unit, rate):
    scaled = upstream * gain
    mean = jnp.mean(scaled, -1, keepdims=True)
    along = jnp.mean(scaled * unit, -1, keepdims=True)
    return rate * (scaled - mean - unit * along)


def flip(array, bit):
    return lax.ppermute(array, "fsdp", [(i, i ^ bit) for i in range(4)])


def swap_core(array):
    return lax.ppermute(array, "core", [(0, 1), (1, 0)])


def gather_rows(shard, parts):
    rows, columns = shard.shape
    if parts != 4:
        return lax.all_gather(shard, "fsdp", axis=0, tiled=True)
    me, core = lax.axis_index("fsdp"), lax.axis_index("core")
    half = rows // 2
    own = lax.dynamic_slice_in_dim(shard, core * half, half, 0)
    near_x, near_y = flip(own, 1), flip(own, 2)
    quarter = half // 2
    far_a = flip(near_x[:quarter], 2)
    far_b = flip(near_y[quarter:], 1)
    held = jnp.zeros((4, half, columns), shard.dtype)
    held = lax.dynamic_update_slice(held, own[None], (me, 0, 0))
    held = lax.dynamic_update_slice(held, near_x[None], (me ^ 1, 0, 0))
    held = lax.dynamic_update_slice(held, near_y[None], (me ^ 2, 0, 0))
    held = lax.dynamic_update_slice(held, far_a[None], (me ^ 3, 0, 0))
    held = lax.dynamic_update_slice(held, far_b[None], (me ^ 3, quarter, 0))
    other = swap_core(held)
    first = jnp.where(core == 0, held, other)
    second = jnp.where(core == 0, other, held)
    return jnp.stack([first, second], 1).reshape(4 * rows, columns)


def reduce_rows(grad, parts):
    rows, columns = grad.shape[0] // parts, grad.shape[1]
    core = lax.axis_index("core")
    half = rows // 2
    split = grad.astype(BF).reshape(parts, 2, half, columns)
    keep = lax.dynamic_index_in_dim(split, core, 1, keepdims=False)
    give = lax.dynamic_index_in_dim(split, 1 - core, 1, keepdims=False)
    pair = (keep.astype(F32) + swap_core(give).astype(F32)).astype(BF)
    spread = lax.all_to_all(pair, "fsdp", 0, 0, tiled=True)
    local = jnp.sum(spread.astype(F32), 0).astype(BF)
    local = lax.psum(local, "z")
    other = swap_core(local)
    first = jnp.where(core == 0, local, other)
    second = jnp.where(core == 0, other, local)
    return jnp.concatenate([first, second], 0).astype(F32)


def on_device(
    images,
    lengths,
    ln1_gain,
    ln1_bias,
    w_qkv,
    qv_bias,
    w_out,
    out_bias,
    ln2_gain,
    ln2_bias,
    w_up,
    up_bias,
    w_down,
    down_bias,
    cotangent,
):
    group, local_tokens, width = images.shape
    parts = lax.axis_size("fsdp")
    seq = lax.axis_size(SEQ)
    share = seq // group
    piece = local_tokens // share
    tokens = seq * piece
    key_count = tokens * share
    scale = HD**-0.5

    def to_image(field):
        moved = lax.all_to_all(field.reshape(seq, piece, width), SEQ, 0, 0, tiled=True)
        return moved.reshape(tokens, width)

    def to_tokens(field):
        moved = lax.all_to_all(field.reshape(seq, piece, width), SEQ, 0, 0, tiled=True)
        return moved.reshape(group, local_tokens, width)

    x_low = to_image(images)
    cot_low = to_image(cotangent)

    vectors = [ln1_gain, ln1_bias, qv_bias[0], qv_bias[1], out_bias, ln2_gain, ln2_bias, down_bias, up_bias]
    sizes = [v.shape[0] for v in vectors]
    packed = lax.all_gather(jnp.concatenate(vectors), "fsdp", axis=0)
    full, at = [], 0
    for size in sizes:
        full.append(packed[:, at : at + size].reshape(1, parts * size).astype(F32))
        at += size
    gain1, shift1, q_bias, v_bias, o_bias, gain2, shift2, d_bias, u_bias = full

    qkv_w = gather_rows(w_qkv, parts)
    out_w = gather_rows(w_out, parts)
    up_w = gather_rows(w_up, parts)
    down_w = gather_rows(w_down.T, parts)

    row = jnp.arange(key_count)
    place = (row % tokens) // piece * local_tokens + row // tokens * piece + row % piece
    image = lax.axis_index(SEQ) // share
    length = lax.dynamic_index_in_dim(lengths, image, 0, keepdims=False)
    bias = jnp.where(place < length, 0.0, -1e30).astype(F32)

    x = x_low.astype(F32)
    unit1, rate1 = normal(x)
    normed1 = (unit1 * gain1 + shift1).astype(BF)
    column_bias = jnp.concatenate([q_bias, jnp.zeros_like(q_bias), v_bias], 1)
    column_scale = jnp.where(jnp.arange(3 * width) < width, scale * LOG2E, 1.0)[None]
    qkv = ((nn(normed1, qkv_w) + column_bias) * column_scale).astype(BF)
    if share == 1:
        keys, values, places = qkv, qkv, (1, 2)
    else:
        both = lax.all_gather(qkv[:, width:], "core", axis=0, tiled=True)
        keys, values, places = both, both, (0, 1)
    attended, lse = attend(qkv, keys, values, places, bias[None])
    residual = x + nn(attended, out_w) + o_bias
    unit2, rate2 = normal(residual)
    normed2 = (unit2 * gain2 + shift2).astype(BF)
    pre = nn(normed2, up_w) + u_bias
    inner = math.sqrt(2 / math.pi)
    tanh = jnp.tanh(inner * (pre + 0.044715 * pre * pre * pre))
    activation = (0.5 * pre * (1 + tanh)).astype(BF)
    slope = 0.5 * (1 + tanh) + 0.5 * pre * (1 - tanh * tanh) * inner * (1 + 3 * 0.044715 * pre * pre)
    slope = slope.astype(BF)
    layer_out = (residual + nt(activation, down_w) + d_bias).astype(BF)
    layer_out = to_tokens(layer_out)

    grad_pre = (nn(cot_low, down_w) * slope).astype(BF)
    grad_down = reduce_rows(tn(cot_low, activation), parts).T
    grad_up = reduce_rows(tn(normed2, grad_pre), parts)
    grad_normed2 = nt(grad_pre, up_w)
    grad_residual = cot_low.astype(F32) + normal_back(grad_normed2, gain2, unit2, rate2)
    grad_branch = grad_residual.astype(BF)
    grad_out = reduce_rows(tn(attended, grad_branch), parts)
    grad_attended = nt(grad_branch, out_w).astype(BF)
    heads = (jnp.arange(width)[:, None] // HD == jnp.arange(H)[None]).astype(F32)
    delta = lax.dot_general(
        heads,
        grad_attended.astype(F32) * attended.astype(F32),
        (((0,), (1,)), ((), ())),
        precision=lax.Precision.HIGHEST,
        preferred_element_type=F32,
    )
    results = attend_back(qkv, keys, values, places, grad_attended, lse, delta, bias[:, None])
    if share == 1:
        (grad_qkv,) = results
    else:
        other = lax.psum_scatter(
            jnp.concatenate(results[1:], 1), "core", scatter_dimension=0, tiled=True
        )
        grad_qkv = jnp.concatenate([results[0], other], 1)
    grad_w_qkv = reduce_rows(tn(normed1, grad_qkv), parts)
    grad_normed1 = nt(grad_qkv, qkv_w)
    grad_images = grad_residual + normal_back(grad_normed1, gain1, unit1, rate1)
    grad_images = to_tokens(grad_images.astype(BF))

    def total(field):
        return jnp.sum(field.astype(F32), 0)

    qkv_sums = total(grad_qkv)
    sums = [
        total(grad_normed1 * unit1),
        total(grad_normed1),
        qkv_sums[:width],
        qkv_sums[2 * width :],
        total(grad_branch),
        total(grad_normed2 * unit2),
        total(grad_normed2),
        total(cot_low),
        total(grad_pre),
    ]
    joined = jnp.concatenate([s.reshape(parts, -1) for s in sums], 1)
    joined = lax.psum(joined, ("fsdp",) + SEQ)
    joined = lax.dynamic_index_in_dim(joined, lax.axis_index("fsdp"), 0, keepdims=False)
    small, at = [], 0
    for size in sizes:
        small.append(joined[at : at + size])
        at += size
    g_gain1, g_shift1, g_q, g_v, g_o, g_gain2, g_shift2, g_d, g_u = small
    return (
        layer_out,
        grad_images,
        g_gain1,
        g_shift1,
        grad_w_qkv,
        jnp.stack([g_q, g_v]),
        grad_out,
        g_o,
        g_gain2,
        g_shift2,
        grad_up,
        g_u,
        grad_down,
        g_d,
    )


def solution(mesh):
    fsdp, seq = mesh.shape["fsdp"], mesh.shape["seq"]
    inner = Mesh(mesh.devices.reshape(fsdp, seq // 2, 2), ("fsdp", "z", "core"))
    tokens = P("fsdp", SEQ, None)
    rows, vector, columns = P("fsdp", None), P("fsdp"), P(None, "fsdp")
    return jax.shard_map(
        on_device,
        mesh=inner,
        in_specs=(
            tokens,
            vector,
            vector,
            vector,
            rows,
            columns,
            rows,
            vector,
            vector,
            vector,
            rows,
            vector,
            columns,
            vector,
            tokens,
        ),
        out_specs=(
            tokens,
            tokens,
            vector,
            vector,
            rows,
            columns,
            rows,
            vector,
            vector,
            vector,
            rows,
            vector,
            columns,
            vector,
        ),
        check_vma=False,
    )
```
